32 devices in a mesh: lat: 8 (over z, core), rad: 4 (over y, x).
Axes of the slice: x: 2, y: 2, z: 4, core: 2. Of those that a mesh axis runs over, the one named last changes fastest.
Arguments:
- residual: float32 [3, 32, 64, 256], P(None, 'rad', 'lat'), may hold values from -30 to 30
- prev_basis: float32 [4, 3, 32, 64, 256], P(None, None, 'rad', 'lat'), may hold values from -30 to 30
- layer_ids: int32 [16, 32, 128], P('rad', 'lat'), may hold values from 0 to 7
- viscosity: float32 [8], replicated, may hold values from 0.1 to 1
- shifts: float32 [4], replicated, may hold values from 0.3 to 2
Outputs:
- new_basis: float32 [4, 3, 32, 64, 256], P(None, None, 'rad', 'lat')
- gram_matrix: float32 [9, 9], replicated
The draws below stay inside these ranges and needn't reach their ends.
All inputs are finite; a program needn't handle non-finite values.
Results may differ from the reference program's by a relative error of at most 0.00019.
Values sent between devices are 32-bit elements; how exact they have to be, the bound alone decides.
No kernel may reach another device: no remote copies, remote signals or barrier semaphores. Data moves between devices by JAX's collectives and lax.ppermute only.
A program may use at most 128 MiB of HBM per device.

```python
import math
import jax
import jax.numpy as jnp
from jax import lax

COMP = 3
S = 4
PREV = 4
LAYERS = 8
ER = 4
EY = 128
BASIS = 9
NRE = 16
NXE = 32
NRN = 32
NXN = 64
NYN = 256
N_RAD = 4


def ramp_field(key, leading):
    full_shape = (leading, COMP, NRN, NXN, NYN)
    radial = (jnp.arange(NRN, dtype=jnp.float32) / NRN)[:, None, None]
    lateral = (jnp.arange(NXN, dtype=jnp.float32) / NXN)[None, :, None]
    across = (jnp.arange(NYN, dtype=jnp.float32) / NYN)[None, None, :]
    smooth = jnp.sin(6.0 * radial + 4.0 * lateral + 3.0 * across + 0.5)
    coef_key = jax.random.fold_in(key, 7)
    coefs = jax.random.truncated_normal(coef_key, -2.0, 2.0, (leading, COMP, 1, 1, 1), jnp.float32)
    noise_vals = jax.random.truncated_normal(key, -4.0, 4.0, full_shape, jnp.float32)
    amplitude = 3.0 ** (radial + lateral - 1.0)
    return (amplitude * (noise_vals + coefs * smooth)).astype(jnp.float32)


def draw_residual(key, part):
    return ramp_field(jax.random.fold_in(key, 11), 1)[0]


def draw_prev_basis(key, part):
    return ramp_field(jax.random.fold_in(key, 23), PREV)


def touch_ends(values, stream_key, low, largest):
    spot = [jax.random.randint(jax.random.fold_in(stream_key, axis), (), 0, length) for axis, length in enumerate(values.shape)]
    widest = values.shape.index(max(values.shape))
    beside = spot[:widest] + [(spot[widest] + 1) % values.shape[widest]] + spot[widest + 1:]
    return values.at[tuple(spot)].set(low).at[tuple(beside)].set(largest)


def setup_inputs(seed: int = 0) -> dict:
    splits = jax.random.split(jax.random.key(seed), 6)
    residual = draw_residual(jax.random.fold_in(splits[5], 71), 0)
    prev_basis = draw_prev_basis(jax.random.fold_in(splits[5], 71), 0)
    layer_ids = touch_ends(jax.random.randint(splits[2], (NRE, NXE, EY), 0, LAYERS), jax.random.fold_in(splits[2], 1), 0, LAYERS - 1).astype(jnp.int32)
    viscosity = jnp.clip(jnp.exp(jax.random.uniform(splits[3], (LAYERS,), jnp.float32, math.log(0.1), math.log(1.0))), 0.1, 1.0)
    shifts = jnp.clip(jax.random.uniform(splits[4], (S,), jnp.float32, 0.3, 2.0), 0.3, 2.0)
    return {"residual": residual, "prev_basis": prev_basis, "layer_ids": layer_ids, "viscosity": viscosity, "shifts": shifts}


stiff_line = ((7.0 / 3, -8.0 / 3, 1.0 / 3), (-8.0 / 3, 16.0 / 3, -8.0 / 3), (1.0 / 3, -8.0 / 3, 7.0 / 3))
mass_line = ((4.0 / 30, 2.0 / 30, -1.0 / 30), (2.0 / 30, 16.0 / 30, 2.0 / 30), (-1.0 / 30, 2.0 / 30, 4.0 / 30))


def contract(line_table, element_vals, axis_pos):
    pieces = [lax.index_in_dim(element_vals, j, axis_pos, keepdims=False) for j in range(3)]
    row_terms = [line_table[i][0] * pieces[0] + line_table[i][1] * pieces[1] + line_table[i][2] * pieces[2] for i in range(3)]
    return jnp.stack(row_terms, axis_pos)


def split_local(field_in, axis_pos):
    el_count = field_in.shape[axis_pos] // 2 - 1
    return jnp.stack([lax.slice_in_dim(field_in, k, k + 2 * el_count - 1, 2, axis_pos) for k in range(3)], 0)


def join_local(element_vals, axis_pos):
    lower_side = element_vals[0]
    middle = element_vals[1]
    upper_side = element_vals[2]
    el_count = lower_side.shape[axis_pos]
    even_nodes = lax.slice_in_dim(lower_side, 1, el_count, 1, axis_pos) + lax.slice_in_dim(upper_side, 0, el_count - 1, 1, axis_pos)
    odd_nodes = lax.slice_in_dim(middle, 1, el_count, 1, axis_pos)
    alternated = jnp.stack([even_nodes, odd_nodes], axis_pos + 1)
    new_shape = list(even_nodes.shape)
    new_shape[axis_pos] = 2 * (el_count - 1)
    return alternated.reshape(new_shape)


def stiffness(field_in, viscous):
    padded = jnp.pad(field_in, ((0, 0), (0, 0), (0, 0), (2, 2)))
    element_vals = split_local(padded, 1)
    element_vals = split_local(element_vals, 3)
    element_vals = split_local(element_vals, 5)
    along_y = contract(mass_line, element_vals, 0)
    mass_rx = contract(mass_line, along_y, 1)
    term_r = contract(stiff_line, mass_rx, 2)
    term_x = contract(mass_line, contract(stiff_line, along_y, 1), 2)
    term_y = contract(stiff_line, contract(mass_line, contract(mass_line, element_vals, 2), 1), 0)
    viscous_wide = jnp.pad(viscous, ((0, 0), (0, 0), (1, 0)))
    weighted = (term_r + term_x + term_y) * viscous_wide
    assembled = join_local(weighted, 5)
    assembled = join_local(assembled, 3)
    return join_local(assembled, 1)


def reference(residual, prev_basis, layer_ids, viscosity, shifts):
    viscous = jnp.take(viscosity, layer_ids)
    eta_pad = jnp.pad(viscous, ((1, 1), (1, 1), (0, 0)))

    def apply_op(field_in):
        padded = jnp.pad(field_in, ((0, 0), (2, 2), (2, 2), (0, 0)))

        def slab_apply(j):
            slab_nodes = lax.dynamic_slice_in_dim(padded, j * (2 * ER), 2 * ER + 4, 1)
            slab_visc = lax.dynamic_slice_in_dim(eta_pad, j * ER, ER + 1, 0)
            return stiffness(slab_nodes, slab_visc[:, :NXE + 1])

        pieces = lax.map(slab_apply, jnp.arange(N_RAD, dtype=jnp.int32))
        return jnp.transpose(pieces, (1, 0, 2, 3, 4)).reshape(field_in.shape)

    vectors = [residual]
    for k in range(S):
        vectors.append(apply_op(vectors[-1]) - shifts[k] * vectors[-1])
    new_basis = jnp.stack(vectors[1:], 0)
    stacked = jnp.concatenate([prev_basis, jnp.stack(vectors, 0)], 0).reshape(BASIS, -1)
    gram_matrix = jnp.dot(stacked, stacked.T, precision=lax.Precision.HIGHEST, preferred_element_type=jnp.float32)
    gram_matrix = gram_matrix / (COMP * NRN * NXN * NYN)
    return new_basis, gram_matrix
```

```python
import functools

import jax
import jax.numpy as jnp
import numpy as np
from jax import lax
from jax.experimental import pallas as pl
from jax.experimental.pallas import tpu as pltpu
from jax.sharding import PartitionSpec as P

C = (1.0 / 36.0, 1.0 / 12.0, 1.0 / 45.0)
LAM = (0.0, 12.0, 60.0)
LANES = 128
VMEM = pl.BlockSpec(memory_space=pltpu.VMEM)
SMEM = pl.BlockSpec(memory_space=pltpu.SMEM)


def mode_weight(i, j, k):
    return C[i] * C[j] * C[k] * (LAM[i] + LAM[j] + LAM[k])


def exact_split(x):
    hi = x.astype(jnp.bfloat16)
    rest = x - hi.astype(jnp.float32)
    mid = rest.astype(jnp.bfloat16)
    low = (rest - mid.astype(jnp.float32)).astype(jnp.bfloat16)
    return hi, mid, low


def right_permute(x, table):
    hi, mid, low = exact_split(x)
    dot = functools.partial(jnp.dot, preferred_element_type=jnp.float32)
    return (dot(hi, table) + dot(mid, table)) + dot(low, table)


def left_permute(table, x):
    hi, mid, low = exact_split(x)
    dot = functools.partial(jnp.dot, preferred_element_type=jnp.float32)
    return (dot(table, hi) + dot(table, mid)) + dot(table, low)


def permutation_tables(comp, node_r, node_x, node_y):
    ex = node_x // 2
    rows = comp * node_r * node_x
    left = np.zeros((rows, rows), np.float32)
    left_back = np.zeros((rows, rows), np.float32)
    for c in range(comp):
        for r in range(node_r):
            for x in range(node_x):
                source = (c * node_r + r) * node_x + x
                target = ((r * 2 + x % 2) * ex + x // 2) * comp + c
                scale = 2.0 ** (r % 2 + x % 2)
                left[target, source] = scale
                left_back[source, target] = 1.0 / scale
    right = np.zeros((node_y, node_y), np.float32)
    right_back = np.zeros((node_y, node_y), np.float32)
    for y in range(node_y):
        target = (y % 2) * (node_y // 2) + y // 2
        right[y, target] = 2.0 ** (y % 2)
        right_back[target, y] = 0.5 ** (y % 2)
    return tuple(jnp.asarray(t, jnp.bfloat16) for t in (left, right, left_back, right_back))


def pack_kernel(head, plane, x_ref, ids_ref, visc_ref, left_ref, right_ref, full_ref, part_ref):
    ids = ids_ref[...]
    viscous = jnp.zeros(ids.shape, jnp.float32)
    for layer in range(visc_ref.shape[0]):
        viscous = jnp.where(ids == layer, visc_ref[layer], viscous)
    full_ref[0:head, :] = viscous
    part_ref[0:head, :] = viscous
    packed = left_permute(left_ref[...], right_permute(x_ref[...], right_ref[...]))
    half = plane // 2
    n_planes = (full_ref.shape[0] - head) // plane
    for p in range(n_planes):
        for parity in range(2):
            piece = packed[p * half : (p + 1) * half, parity * LANES : (parity + 1) * LANES]
            start = head + p * plane + parity * half
            full_ref[start : start + half, :] = piece
            if start + half <= part_ref.shape[0]:
                part_ref[start : start + half, :] = piece


def pair_list(first, count):
    return [(i, j) for j in range(first, count) for i in range(j + 1)]


def known_gram_kernel(n_prev, prev_ref, x_ref, out_ref):
    rows = x_ref.shape[0]
    pairs = pair_list(0, n_prev + 1)

    def body(t, sums):
        for half in range(2):
            vecs = []
            lanes = slice(half * LANES, (half + 1) * LANES)
            for q in range(n_prev):
                vecs.append(prev_ref[q, pl.ds(pl.multiple_of(t * 8, 8), 8), lanes])
            vecs.append(x_ref[pl.ds(pl.multiple_of(t * 8, 8), 8), lanes])
            sums = tuple(s + vecs[i] * vecs[j] for s, (i, j) in zip(sums, pairs))
        return sums

    zero = jnp.zeros((8, LANES), jnp.float32)
    sums = lax.fori_loop(0, rows // 8, body, tuple(zero for _ in pairs))
    for q, s in enumerate(sums):
        out_ref[q] = s


def main_kernel(
    geo,
    own_ref,
    lo_ref,
    hi_ref,
    left_own_ref,
    right_own_ref,
    left_pair_ref,
    right_pair_ref,
    known_ref,
    prev_ref,
    x_ref,
    shifts_ref,
    left_table_ref,
    right_table_ref,
    basis_ref,
    gram_ref,
    field_a,
    field_b,
    carry_x,
    eta_ref,
    flat_ref,
    sums_ref,
):
    comp, er, ex, steps, n_prev, head, plane = geo
    quarter = plane // 4
    full_rows = own_ref.shape[0]
    last_rad = lax.axis_index("rad") == lax.axis_size("rad") - 1
    last_lat = lax.axis_index("lat") == lax.axis_size("lat") - 1

    columns = (
        ((left_pair_ref, 0), (left_own_ref, 0), (left_pair_ref, full_rows)),
        ((lo_ref, 0), (own_ref, 0), (hi_ref, 0)),
        ((right_pair_ref, 0), (right_own_ref, 0), (right_pair_ref, full_rows)),
    )
    n_planes = 2 * er
    for column, blocks in enumerate(columns):
        for slab, (ref, base) in enumerate(blocks):
            count = n_planes - 1 if slab == 2 else n_planes
            for p in range(count):
                for py in range(2):
                    for px in range(2):
                        start = base + head + p * plane + (py * 2 + px) * quarter
                        field_a[
                            slab * n_planes + p,
                            py,
                            px,
                            column * quarter : (column + 1) * quarter,
                            :,
                        ] = ref[start : start + quarter, :]
            for a in range(er):
                piece = ref[base + a * ex : base + (a + 1) * ex, :]
                for c in range(comp):
                    eta_ref[
                        slab * er + a, pl.ds(column * quarter + c, ex, stride=comp), :
                    ] = piece

    lane = lax.broadcasted_iota(jnp.int32, (8, LANES), 1)
    not_first = lane != 0
    not_last = lane != LANES - 1

    def forward_line(e0, odd, e1):
        s = e0 + e1
        up = s + odd
        return up + odd, e0 - e1, s - odd

    def backward_line(g0, g1, g2):
        p = g0 + g2
        return p + g1, (g0 + g0) - g2, p - g1

    def forward_plane(src, p, b):
        modes = []
        for py in range(2):
            modes.append(
                forward_line(
                    src[p, py, 0, pl.ds(b, 8), :],
                    src[p, py, 1, pl.ds(b, 8), :],
                    src[p, py, 0, pl.ds(b + comp, 8), :],
                )
            )
        out = []
        for i in range(3):
            even = modes[0][i]
            after = jnp.where(not_last, pltpu.roll(even, LANES - 1, 1), 0.0)
            out.append(forward_line(even, modes[1][i], after))
        return out

    def backward_plane(src, dst, p, b, modes, shift, scale):
        evens, odds = [], []
        for i in range(3):
            low, odd, high = backward_line(*modes[i])
            evens.append(low + jnp.where(not_first, pltpu.roll(high, 1, 1), 0.0))
            odds.append(odd)
        for py, line in enumerate((evens, odds)):
            low, odd, high = backward_line(*line)
            carry_x[p, py, pl.ds(b + comp, 8), :] = high
            even = low + carry_x[p, py, pl.ds(b, 8), :]
            factor = scale * 4.0**py
            if factor != 1.0:
                even = even * factor
            dst[p, py, 0, pl.ds(b, 8), :] = even - shift * src[p, py, 0, pl.ds(b, 8), :]
            dst[p, py, 1, pl.ds(b, 8), :] = (
                odd * (factor * 4.0) - shift * src[p, py, 1, pl.ds(b, 8), :]
            )

    fields = (field_a, field_b)
    offset_r, offset_x = er - steps, ex - steps
    for k in range(steps):
        src, dst = fields[k % 2], fields[(k + 1) % 2]
        shift = shifts_ref[k]
        first_r = offset_r + k
        last_r = 2 * er + steps - 2 - k
        first_x = offset_x + k
        n_x = 2 * ex + steps - 1 - k - first_x
        n_tiles = -(-n_x * comp // 8)
        for tile in range(n_tiles):
            b = first_x * comp + tile * 8
            front = forward_plane(src, 2 * first_r, b)
            carried = None
            for a in range(first_r, last_r + 1):
                middle = forward_plane(src, 2 * a + 1, b)
                back = forward_plane(src, 2 * a + 2, b)
                eta = eta_ref[a, pl.ds(b, 8), :]
                weights = {}
                even_modes = [[None] * 3 for _ in range(3)]
                odd_modes = [[None] * 3 for _ in range(3)]
                next_carry = [[None] * 3 for _ in range(3)]
                for i in range(3):
                    for j in range(3):
                        t0, t1, t2 = forward_line(front[i][j], middle[i][j], back[i][j])
                        g = []
                        for q, t in enumerate((t0, t1, t2)):
                            key = tuple(sorted((q, i, j)))
                            if key == (0, 0, 0):
                                g.append(None)
                                continue
                            if key not in weights:
                                weights[key] = eta * mode_weight(*key)
                            g.append(t * weights[key])
                        if g[0] is None:
                            low, odd, high = g[2] + g[1], -g[2], g[2] - g[1]
                        else:
                            low, odd, high = backward_line(*g)
                        even_modes[i][j] = low if carried is None else low + carried[i][j]
                        odd_modes[i][j] = odd
                        next_carry[i][j] = high
                if a > first_r:
                    backward_plane(src, dst, 2 * a, b, even_modes, shift, 1.0)
                backward_plane(src, dst, 2 * a + 1, b, odd_modes, shift, 4.0)
                carried = next_carry
                front = back

        if k < steps - 1:

            @pl.when(last_rad)
            def _():
                dst[4 * er] = jnp.zeros(dst.shape[1:], jnp.float32)

            @pl.when(last_lat)
            def _():
                top = 2 * quarter
                zeros = jnp.zeros((comp, LANES), jnp.float32)
                for p in range(2 * first_r + 1, 2 * last_r + 1):
                    for py in range(2):
                        dst[p, py, 0, top : top + comp, :] = zeros

        for p in range(n_planes):
            for py in range(2):
                for px in range(2):
                    start = (p * 2 + px) * quarter
                    flat_ref[start : start + quarter, py * LANES : (py + 1) * LANES] = dst[
                        n_planes + p, py, px, quarter : 2 * quarter, :
                    ]
        basis_ref[k] = right_permute(
            left_permute(left_table_ref[...], flat_ref[...]), right_table_ref[...]
        )

    n_known = n_prev + 1
    total = n_known + steps
    pairs = pair_list(n_known, total)

    def body(t, sums):
        rows = pl.ds(pl.multiple_of(t * 8, 8), 8)
        for half in range(2):
            lanes = slice(half * LANES, (half + 1) * LANES)
            vecs = [prev_ref[q, rows, lanes] for q in range(n_prev)]
            vecs.append(x_ref[rows, lanes])
            vecs += [basis_ref[q, rows, lanes] for q in range(steps)]
            sums = tuple(s + vecs[i] * vecs[j] for s, (i, j) in zip(sums, pairs))
        return sums

    zero = jnp.zeros((8, LANES), jnp.float32)
    sums = lax.fori_loop(0, x_ref.shape[0] // 8, body, tuple(zero for _ in pairs))
    sums = [known_ref[q] for q in range(len(pair_list(0, n_known)))] + list(sums)
    sums_ref[...] = jnp.zeros(sums_ref.shape, jnp.float32)
    for s, (i, j) in zip(sums, pair_list(0, n_known) + pairs):
        row = jnp.sum(s, axis=0, keepdims=True)
        sums_ref[i * total + j : i * total + j + 1, :] = row
        if i != j:
            sums_ref[j * total + i : j * total + i + 1, :] = row
    ones = jnp.ones((8, LANES), jnp.float32)
    gram_ref[...] = lax.dot_general(
        ones,
        sums_ref[...],
        (((1,), (1,)), ((), ())),
        precision=lax.Precision.HIGHEST,
        preferred_element_type=jnp.float32,
    )


def finish_kernel(total, dof_count, parts_ref, out_ref):
    row = jnp.sum(parts_ref[...], axis=0, keepdims=True) / dof_count
    for i in range(total):
        out_ref[i : i + 1, :] = row[:, i * total : (i + 1) * total]


def shifted(value, axis, step):
    count = lax.axis_size(axis)
    if step > 0:
        return lax.ppermute(value, axis, [(i, i + 1) for i in range(count - 1)])
    return lax.ppermute(value, axis, [(i + 1, i) for i in range(count - 1)])


def on_device(residual, prev_basis, layer_ids, viscosity, shifts):
    comp, node_r, node_x, node_y = residual.shape
    steps, n_prev = shifts.shape[0], prev_basis.shape[0]
    er, ex = node_r // 2, node_x // 2
    n_devices = lax.axis_size("rad") * lax.axis_size("lat")
    total = n_prev + 1 + steps
    assert node_y == 2 * LANES and steps <= min(er, ex) and total * total <= LANES
    rows = comp * node_r * node_x
    quarter = ex * comp
    plane = 4 * quarter
    head = er * ex
    full_rows = head + node_r * plane
    part_rows = full_rows - plane
    f32 = jnp.float32
    left, right, left_back, right_back = permutation_tables(comp, node_r, node_x, node_y)

    x = residual.reshape(rows, node_y)
    prev = prev_basis.reshape(n_prev, rows, node_y)
    full, part = pl.pallas_call(
        functools.partial(pack_kernel, head, plane),
        out_shape=(
            jax.ShapeDtypeStruct((full_rows, LANES), f32),
            jax.ShapeDtypeStruct((part_rows, LANES), f32),
        ),
        in_specs=[VMEM, VMEM, SMEM, VMEM, VMEM],
        out_specs=(VMEM, VMEM),
        name="pack",
    )(x, layer_ids.reshape(head, LANES), viscosity, left, right)

    lo = shifted(full, "rad", 1)
    hi = shifted(part, "rad", -1)
    left_own = shifted(full, "lat", 1)
    right_own = shifted(full, "lat", -1)
    known = pl.pallas_call(
        functools.partial(known_gram_kernel, n_prev),
        out_shape=jax.ShapeDtypeStruct((len(pair_list(0, n_prev + 1)), 8, LANES), f32),
        in_specs=[VMEM, VMEM],
        out_specs=VMEM,
        cost_estimate=pl.CostEstimate(
            flops=4000000, bytes_accessed=4 * (n_prev + 1) * rows * node_y, transcendentals=0
        ),
        name="known_gram",
    )(prev, x)
    both = jnp.concatenate([lo, hi], 0)
    left_pair = shifted(both, "lat", 1)
    right_pair = shifted(both, "lat", -1)

    width = -(-(3 * quarter + comp + 8) // 8) * 8
    geo = (comp, er, ex, steps, n_prev, head, plane)
    field = pltpu.VMEM((3 * node_r, 2, 2, width, LANES), f32)
    basis, gram = pl.pallas_call(
        functools.partial(main_kernel, geo),
        out_shape=(
            jax.ShapeDtypeStruct((steps, rows, node_y), f32),
            jax.ShapeDtypeStruct((8, LANES), f32),
        ),
        in_specs=[VMEM] * 10 + [SMEM, VMEM, VMEM],
        out_specs=(VMEM, VMEM),
        scratch_shapes=[
            field,
            field,
            pltpu.VMEM((3 * node_r, 2, width, LANES), f32),
            pltpu.VMEM((3 * er, width, LANES), f32),
            pltpu.VMEM((rows, node_y), f32),
            pltpu.VMEM((LANES, LANES), f32),
        ],
        name="powers",
    )(
        full, lo, hi, left_own, right_own, left_pair, right_pair, known, prev, x, shifts,
        left_back, right_back,
    )

    spread = jnp.broadcast_to(gram[:1][None], (n_devices, 1, LANES))
    parts = lax.all_to_all(spread, ("rad", "lat"), 0, 0)
    dof_count = rows * node_y * n_devices
    gram_matrix = pl.pallas_call(
        functools.partial(finish_kernel, total, float(dof_count)),
        out_shape=jax.ShapeDtypeStruct((total, total), f32),
        in_specs=[VMEM],
        out_specs=VMEM,
        name="finish",
    )(parts.reshape(n_devices, LANES))
    return basis.reshape((steps,) + residual.shape), gram_matrix


def solution(mesh):
    placed = (
        P(None, "rad", "lat", None),
        P(None, None, "rad", "lat", None),
        P("rad", "lat", None),
        P(),
        P(),
    )
    return jax.shard_map(
        on_device,
        mesh=mesh,
        in_specs=placed,
        out_specs=(P(None, None, "rad", "lat", None), P()),
        check_vma=False,
    )
```
